32 devices in a mesh: zero: 8 (over y, x, core), width: 4 (over z).
Axes of the slice: x: 2, y: 2, z: 4, core: 2. Of those that a mesh axis runs over, the one named last changes fastest.
Arguments:
- w_gate: bfloat16 [3072, 8192], P('zero', 'width'), may hold values from -0.109375 to 0.109375
- low_gate: bfloat16 [3072, 16], P('zero'), may hold values from -0.109375 to 0.109375
- high_gate: bfloat16 [16, 8192], P(None, 'width'), may hold values from -1.5 to 1.5
- w_up: bfloat16 [3072, 8192], P('zero', 'width'), may hold values from -0.109375 to 0.109375
- low_up: bfloat16 [3072, 16], P('zero'), may hold values from -0.109375 to 0.109375
- high_up: bfloat16 [16, 8192], P(None, 'width'), may hold values from -1.5 to 1.5
- norm_train: float32 [3072], P(('zero', 'width')), may hold values from 0.25 to 1.75
- norm_step: float32 [3072], P(('zero', 'width')), may hold values from -0.3 to 0.3
Outputs:
- serving_gate: bfloat16 [8192, 3072], P('width')
- serving_up: bfloat16 [8192, 3072], P('width')
- serve_norm: bfloat16 [3072], replicated
The draws below stay inside these ranges and needn't reach their ends.
All inputs are finite; a program needn't handle non-finite values.
Results may differ from the reference program's by a relative error of at most 0.001.
Values may be sent and summed in bfloat16 or wider, within the bound.
A program may use at most 128 MiB of HBM per device.

```python
import jax
import jax.numpy as jnp

D_MODEL = 3072
D_INNER = 8192
RANK = 16


def block_scale(own_key, shape, split, smallest, largest):
    level, own = 1.0, jax.random.fold_in(own_key, 6)
    for axis_at, parts in split:
        steps = jnp.exp(jax.random.uniform(jax.random.fold_in(own, axis_at), (parts,), jnp.float32, smallest / len(split), largest / len(split)))
        level = level * jnp.repeat(steps, shape[axis_at] // parts).reshape([-1 if axis == axis_at else 1 for axis in range(len(shape))])
    return level


def bell_draw(rng, shape, width, bound, shards=(), held_as=jnp.bfloat16):
    result = jax.random.normal(rng, shape, jnp.float32) * width
    if len(shards) > 0:
        result = block_scale(rng, shape, shards, -0.22, 0.18) * result
    return jnp.clip(result, min=-bound, max=bound).astype(held_as)


def setup_inputs(seed: int = 0) -> dict:
    streams_of = jax.random.split(jax.random.key(seed), 9)
    return {
        "w_gate": bell_draw(streams_of[0], (D_MODEL, D_INNER), D_MODEL ** -0.5, 0.109375, ((0, 8), (1, 4))),
        "low_gate": bell_draw(streams_of[1], (D_MODEL, RANK), D_MODEL ** -0.5, 0.109375, ((0, 8),)),
        "high_gate": bell_draw(streams_of[2], (RANK, D_INNER), RANK ** -0.5, 1.5, ((1, 4),)),
        "w_up": bell_draw(streams_of[3], (D_MODEL, D_INNER), D_MODEL ** -0.5, 0.109375, ((0, 8), (1, 4))),
        "low_up": bell_draw(streams_of[4], (D_MODEL, RANK), D_MODEL ** -0.5, 0.109375, ((0, 8),)),
        "high_up": bell_draw(streams_of[5], (RANK, D_INNER), RANK ** -0.5, 1.5, ((1, 4),)),
        "norm_train": jnp.clip(1.0 + 0.15 * jax.random.normal(streams_of[6], (D_MODEL,), jnp.float32), 0.25, 1.75),
        "norm_step": jnp.clip(jax.random.uniform(streams_of[7], (D_MODEL,), jnp.float32, -0.3, 0.3) * block_scale(streams_of[7], (D_MODEL,), ((0, 32),), -0.4, 0.0), -0.3, 0.3),
    }


mix_rate = 1.0


def reference(w_gate, low_gate, high_gate, w_up, low_up, high_up, norm_train, norm_step):
    whole_gate = w_gate.astype(jnp.float32) + mix_rate * jnp.dot(low_gate, high_gate, preferred_element_type=jnp.float32)
    whole_up = w_up.astype(jnp.float32) + mix_rate * jnp.dot(low_up, high_up, preferred_element_type=jnp.float32)
    serving_gate = whole_gate.T.astype(jnp.bfloat16)
    serving_up = whole_up.T.astype(jnp.bfloat16)
    serve_norm = (norm_train + norm_step).astype(jnp.bfloat16)
    return serving_gate, serving_up, serve_norm
```

```python
import functools

import jax
import jax.numpy as jnp
from jax import lax
from jax.experimental import pallas as pl
from jax.experimental.pallas import tpu as pltpu
from jax.sharding import PartitionSpec as P

mix_rate = 1.0
MESH = pl.DeviceIdType.MESH
CHUNK = 256


def merge_kernel(
    n_zero, n_width, w_gate, low_gate, high_gate, w_up, low_up, high_up, step_a, step_b,
    held, gains, w, low, high, gain, load_sem, gain_send, gain_recv, send_sem, recv_sem,
):
    zero, width = lax.axis_index("zero"), lax.axis_index("width")
    core = lax.rem(zero, 2)
    partner = zero + 1 - 2 * core
    chip = zero // 2
    cx, cy = lax.rem(chip, 2), chip // 2
    over_x = zero + 2 * (1 - 2 * cx)
    over_y = zero + 4 * (1 - 2 * cy)
    first = over_x + core * (over_y - over_x)
    second = over_y + core * (over_x - over_y)
    across = over_x + over_y - zero
    their_first = second + partner - zero
    their_second = first + partner - zero
    their_across = across + partner - zero

    loads = [
        pltpu.make_async_copy(src, dst, load_sem.at[i])
        for i, (src, dst) in enumerate(
            [
                (w_gate, w.at[0]), (low_gate, low.at[0]), (high_gate, high.at[0]),
                (w_up, w.at[1]), (low_up, low.at[1]), (high_up, high.at[1]),
            ]
        )
    ]
    for load in loads:
        load.start()
    gain[...] = step_a[...] + step_b[...]

    n = n_zero * n_width
    flat = zero * n_width + width

    def other(d):
        t = lax.rem(flat + d, n)
        return {"zero": t // n_width, "width": lax.rem(t, n_width)}

    barrier = pltpu.get_barrier_semaphore()

    def greet(d, _):
        pl.semaphore_signal(barrier, inc=1, device_id=other(d), device_id_type=MESH)
        return _

    lax.fori_loop(1, n, greet, 0)
    gains[flat] = gain[...]
    for load in loads:
        load.wait()

    rows = held.shape[2]
    per = rows // CHUNK
    count = 2 * per

    def at(block, i):
        return held.at[block, i // per, pl.ds(pl.multiple_of(lax.rem(i, per) * CHUNK, CHUNK), CHUNK)]

    def make(i):
        a = i // per
        cols = pl.ds(pl.multiple_of(lax.rem(i, per) * CHUNK, CHUNK), CHUNK)
        delta = lax.dot_general(
            high[a, :, cols], low[a], (((0,), (0,)), ((), ())),
            preferred_element_type=jnp.float32,
        )
        base = w[a, :, cols].T.astype(jnp.float32)
        held[zero, a, cols] = (base + mix_rate * delta).astype(held.dtype)

    def copy(flow, block, i, target):
        return pltpu.make_async_remote_copy(
            src_ref=at(block, i), dst_ref=at(block, i),
            send_sem=send_sem.at[flow, i], recv_sem=recv_sem.at[flow, i],
            device_id={"zero": target}, device_id_type=MESH,
        )

    def send_own(i):
        copy(1, zero, i, first).start()
        copy(2, zero, i, second).start()
        copy(0, zero, i, partner).start()

    make(0)
    pl.semaphore_wait(barrier, n - 1)

    def make_and_send(i, _):
        make(i)
        send_own(i - 1)
        return _

    lax.fori_loop(1, count, make_and_send, 0)
    send_own(count - 1)

    def gain_copy(d, slot):
        return pltpu.make_async_remote_copy(
            src_ref=gain, dst_ref=gains.at[slot],
            send_sem=gain_send.at[d], recv_sem=gain_recv.at[d],
            device_id=other(d), device_id_type=MESH,
        )

    def send_gain(d, _):
        gain_copy(d, flat).start()
        return _

    lax.fori_loop(1, n, send_gain, 0)

    def relay(i, _):
        copy(1, first, i, first).wait_recv()
        copy(3, first, i, second).start()
        copy(4, first, i, partner).start()
        copy(2, second, i, second).wait_recv()
        copy(5, second, i, partner).start()
        return _

    lax.fori_loop(0, count, relay, 0)

    def pass_on(i, _):
        copy(3, across, i, second).wait_recv()
        copy(6, across, i, partner).start()
        return _

    lax.fori_loop(0, count, pass_on, 0)

    def end_gain(d, _):
        gain_copy(d, lax.rem(flat + n - d, n)).wait()
        return _

    lax.fori_loop(1, n, end_gain, 0)

    def end(i, _):
        copy(0, partner, i, partner).wait_recv()
        copy(4, their_first, i, partner).wait_recv()
        copy(5, their_second, i, partner).wait_recv()
        copy(6, their_across, i, partner).wait_recv()
        copy(0, zero, i, partner).wait_send()
        copy(1, zero, i, first).wait_send()
        copy(2, zero, i, second).wait_send()
        copy(3, first, i, second).wait_send()
        copy(4, first, i, partner).wait_send()
        copy(5, second, i, partner).wait_send()
        copy(6, across, i, partner).wait_send()
        return _

    lax.fori_loop(0, count, end, 0)


def flush_kernel(held, out_gate, out_up, sem):
    blocks, _, _, depth = held.shape
    copies = [
        pltpu.make_async_copy(
            held.at[b, a], out.at[:, pl.ds(b * depth, depth)], sem.at[b, a]
        )
        for a, out in enumerate((out_gate, out_up))
        for b in range(blocks)
    ]
    for c in copies:
        c.start()
    for c in copies:
        c.wait()


def by_kernels(n_zero, n_width, w_gate, low_gate, high_gate, w_up, low_up, high_up, norm_train, norm_step):
    depth, rows = w_gate.shape
    rank = high_gate.shape[0]
    share = norm_train.shape[0]
    n = n_zero * n_width
    count = 2 * (rows // CHUNK)
    anywhere = pl.BlockSpec(memory_space=pl.ANY)
    vmem = pl.BlockSpec(memory_space=pltpu.VMEM)
    dma = pltpu.SemaphoreType.DMA
    held, gains = pl.pallas_call(
        functools.partial(merge_kernel, n_zero, n_width),
        out_shape=(
            pltpu.VMEM((n_zero, 2, rows, depth), jnp.bfloat16),
            pltpu.VMEM((n, 1, share), jnp.float32),
        ),
        in_specs=[anywhere] * 6 + [vmem] * 2,
        out_specs=(vmem, vmem),
        scratch_shapes=[
            pltpu.VMEM((2, depth, rows), jnp.bfloat16),
            pltpu.VMEM((2, rank, depth), jnp.bfloat16),
            pltpu.VMEM((2, rank, rows), jnp.bfloat16),
            pltpu.VMEM((1, share), jnp.float32),
            dma((6,)),
            dma((n,)),
            dma((n,)),
            dma((7, count)),
            dma((7, count)),
        ],
        compiler_params=pltpu.CompilerParams(
            collective_id=0, has_side_effects=True, vmem_limit_bytes=34 * 2**20
        ),
    )(
        w_gate, low_gate.T, high_gate, w_up, low_up.T, high_up,
        norm_train.reshape(1, share), norm_step.reshape(1, share),
    )
    out = jax.ShapeDtypeStruct((rows, n_zero * depth), jnp.bfloat16)
    serving_gate, serving_up = pl.pallas_call(
        flush_kernel,
        out_shape=(out, out),
        in_specs=[vmem],
        out_specs=(anywhere, anywhere),
        scratch_shapes=[dma((n_zero, 2))],
        compiler_params=pltpu.CompilerParams(vmem_limit_bytes=34 * 2**20),
    )(pltpu.with_memory_space_constraint(held, pltpu.VMEM))
    return serving_gate, serving_up, gains.reshape(n * share).astype(jnp.bfloat16)


def by_gathers(w_gate, low_gate, high_gate, w_up, low_up, high_up, norm_train, norm_step):
    def merged(w, low, high):
        whole = w.astype(jnp.float32) + mix_rate * jnp.dot(
            low, high, preferred_element_type=jnp.float32
        )
        return lax.all_gather(whole.astype(jnp.bfloat16), "zero", axis=0, tiled=True).T

    serve_norm = lax.all_gather(
        (norm_train + norm_step).astype(jnp.bfloat16), ("zero", "width"), axis=0, tiled=True
    )
    return merged(w_gate, low_gate, high_gate), merged(w_up, low_up, high_up), serve_norm


def solution(mesh):
    n_zero, n_width = mesh.shape["zero"], mesh.shape["width"]
    planar = n_zero == 2 * 2 * 2
    body = functools.partial(by_kernels, n_zero, n_width) if planar else by_gathers
    placed = (
        P("zero", "width"),
        P("zero", None),
        P(None, "width"),
        P("zero", "width"),
        P("zero", None),
        P(None, "width"),
        P(("zero", "width")),
        P(("zero", "width")),
    )
    return jax.shard_map(
        body,
        mesh=mesh,
        in_specs=placed,
        out_specs=(P("width", None), P("width", None), P()),
        check_vma=False,
    )
```

```python
import functools

import jax
import jax.numpy as jnp
from jax import lax
from jax.experimental import pallas as pl
from jax.experimental.pallas import tpu as pltpu
from jax.sharding import PartitionSpec as P

mix_rate = 1.0
MESH = pl.DeviceIdType.MESH
PIECES = 4


def merge_kernel(
    n_zero, n_width, w_gate, low_gate, high_gate, w_up, low_up, high_up, step_a, step_b,
    held, gains, w, low, high, load_sem, gain_send, gain_recv, send_sem, recv_sem,
):
    zero, width = lax.axis_index("zero"), lax.axis_index("width")
    core = lax.rem(zero, 2)
    partner = zero + 1 - 2 * core
    chip = zero // 2
    cx, cy = lax.rem(chip, 2), chip // 2
    over_x = zero + 2 * (1 - 2 * cx)
    over_y = zero + 4 * (1 - 2 * cy)
    first = over_x + core * (over_y - over_x)
    second = over_y + core * (over_x - over_y)
    across = over_x + over_y - zero
    their_first = second + partner - zero
    their_second = first + partner - zero
    their_across = across + partner - zero

    flat = zero * n_width + width
    spans = [1 << b for b in range(n_width.bit_length() - 1)]

    def beside(span):
        return width + span * (1 - 2 * lax.rem(width // span, 2))

    barrier = pltpu.get_barrier_semaphore()
    for target in (partner, first, second):
        pl.semaphore_signal(barrier, inc=1, device_id={"zero": target}, device_id_type=MESH)
    for span in spans:
        pl.semaphore_signal(barrier, inc=1, device_id={"width": beside(span)}, device_id_type=MESH)

    loads = [
        pltpu.make_async_copy(src, dst, load_sem.at[i])
        for i, (src, dst) in enumerate(
            [
                (w_gate, w.at[0]), (low_gate, low.at[0]), (high_gate, high.at[0]),
                (w_up, w.at[1]), (low_up, low.at[1]), (high_up, high.at[1]),
            ]
        )
    ]
    for load in loads:
        load.start()
    gains[flat] = step_a[...] + step_b[...]
    for load in loads[:3]:
        load.wait()

    rows = held.shape[2]
    per = PIECES
    chunk = rows // per
    count = 2 * per

    def at(block, i):
        return held.at[block, i // per, pl.ds(pl.multiple_of(lax.rem(i, per) * chunk, chunk), chunk)]

    def make(i):
        a = i // per
        cols = pl.ds(pl.multiple_of(lax.rem(i, per) * chunk, chunk), chunk)
        delta = lax.dot_general(
            high[a, :, cols], low[a], (((0,), (0,)), ((), ())),
            preferred_element_type=jnp.float32,
        )
        base = w[a, :, cols].T.astype(jnp.float32)
        held[zero, a, cols] = (base + mix_rate * delta).astype(held.dtype)

    def copy(flow, block, i, target):
        return pltpu.make_async_remote_copy(
            src_ref=at(block, i), dst_ref=at(block, i),
            send_sem=send_sem.at[flow, i], recv_sem=recv_sem.at[flow, i],
            device_id={"zero": target}, device_id_type=MESH,
        )

    def send_own(i):
        copy(1, zero, i, first).start()
        copy(2, zero, i, second).start()
        copy(0, zero, i, partner).start()

    make(0)
    make(1)
    pl.semaphore_wait(barrier, 3 + len(spans))
    send_own(0)
    for load in loads[3:]:
        load.wait()

    def make_and_send(i, _):
        make(i)
        send_own(i - 1)
        return _

    lax.fori_loop(2, count, make_and_send, 0)
    send_own(count - 1)

    def gain_beside(b, start):
        span = spans[b]
        own = gains.at[pl.ds(start // span * span, span)]
        return pltpu.make_async_remote_copy(
            src_ref=own, dst_ref=own, send_sem=gain_send.at[b], recv_sem=gain_recv.at[b],
            device_id={"width": beside(span)}, device_id_type=MESH,
        )

    for b, span in enumerate(spans):
        gain_beside(b, flat).start()
        gain_beside(b, zero * n_width + beside(span)).wait_recv()

    def gain_copy(flow, block, target):
        part = gains.at[pl.ds(block * n_width, n_width)]
        return pltpu.make_async_remote_copy(
            src_ref=part, dst_ref=part,
            send_sem=send_sem.at[flow, count], recv_sem=recv_sem.at[flow, count],
            device_id={"zero": target}, device_id_type=MESH,
        )

    gain_copy(1, zero, first).start()
    gain_copy(2, zero, second).start()
    gain_copy(0, zero, partner).start()

    def relay(i, _):
        copy(1, first, i, first).wait_recv()
        copy(3, first, i, second).start()
        copy(4, first, i, partner).start()
        copy(2, second, i, second).wait_recv()
        copy(5, second, i, partner).start()
        return _

    lax.fori_loop(0, count, relay, 0)
    gain_copy(1, first, first).wait_recv()
    gain_copy(3, first, second).start()
    gain_copy(4, first, partner).start()
    gain_copy(2, second, second).wait_recv()
    gain_copy(5, second, partner).start()

    def pass_on(i, _):
        copy(3, across, i, second).wait_recv()
        copy(6, across, i, partner).start()
        return _

    lax.fori_loop(0, count, pass_on, 0)
    gain_copy(3, across, second).wait_recv()
    gain_copy(6, across, partner).start()

    for flow, block in ((0, partner), (4, their_first), (5, their_second), (6, their_across)):
        gain_copy(flow, block, partner).wait_recv()
    for flow, block in enumerate((zero, zero, zero, first, first, second, across)):
        gain_copy(flow, block, partner).wait_send()
    for b in range(len(spans)):
        gain_beside(b, flat).wait_send()

    def end(i, _):
        copy(0, partner, i, partner).wait_recv()
        copy(4, their_first, i, partner).wait_recv()
        copy(5, their_second, i, partner).wait_recv()
        copy(6, their_across, i, partner).wait_recv()
        copy(0, zero, i, partner).wait_send()
        copy(1, zero, i, first).wait_send()
        copy(2, zero, i, second).wait_send()
        copy(3, first, i, second).wait_send()
        copy(4, first, i, partner).wait_send()
        copy(5, second, i, partner).wait_send()
        copy(6, across, i, partner).wait_send()
        return _

    lax.fori_loop(0, count, end, 0)


def flush_kernel(held, out_gate, out_up, sem):
    blocks, _, _, depth = held.shape
    copies = [
        pltpu.make_async_copy(
            held.at[b, a], out.at[:, pl.ds(b * depth, depth)], sem.at[b, a]
        )
        for a, out in enumerate((out_gate, out_up))
        for b in range(blocks)
    ]
    for c in copies:
        c.start()
    for c in copies:
        c.wait()


def by_kernels(n_zero, n_width, w_gate, low_gate, high_gate, w_up, low_up, high_up, norm_train, norm_step):
    depth, rows = w_gate.shape
    rank = high_gate.shape[0]
    share = norm_train.shape[0]
    n = n_zero * n_width
    count = 2 * PIECES
    anywhere = pl.BlockSpec(memory_space=pl.ANY)
    vmem = pl.BlockSpec(memory_space=pltpu.VMEM)
    dma = pltpu.SemaphoreType.DMA
    held, gains = pl.pallas_call(
        functools.partial(merge_kernel, n_zero, n_width),
        out_shape=(
            pltpu.VMEM((n_zero, 2, rows, depth), jnp.bfloat16),
            pltpu.VMEM((n, 1, share), jnp.float32),
        ),
        in_specs=[anywhere] * 6 + [vmem] * 2,
        out_specs=(vmem, vmem),
        scratch_shapes=[
            pltpu.VMEM((2, depth, rows), jnp.bfloat16),
            pltpu.VMEM((2, rank, depth), jnp.bfloat16),
            pltpu.VMEM((2, rank, rows), jnp.bfloat16),
            dma((6,)),
            dma((n_width.bit_length(),)),
            dma((n_width.bit_length(),)),
            dma((7, count + 1)),
            dma((7, count + 1)),
        ],
        compiler_params=pltpu.CompilerParams(
            collective_id=0, has_side_effects=True, vmem_limit_bytes=34 * 2**20
        ),
    )(
        w_gate, low_gate.T, high_gate, w_up, low_up.T, high_up,
        norm_train.reshape(1, share), norm_step.reshape(1, share),
    )
    out = jax.ShapeDtypeStruct((rows, n_zero * depth), jnp.bfloat16)
    serving_gate, serving_up = pl.pallas_call(
        flush_kernel,
        out_shape=(out, out),
        in_specs=[vmem],
        out_specs=(anywhere, anywhere),
        scratch_shapes=[dma((n_zero, 2))],
        compiler_params=pltpu.CompilerParams(vmem_limit_bytes=34 * 2**20),
    )(pltpu.with_memory_space_constraint(held, pltpu.VMEM))
    return serving_gate, serving_up, gains.reshape(n * share).astype(jnp.bfloat16)


def by_gathers(w_gate, low_gate, high_gate, w_up, low_up, high_up, norm_train, norm_step):
    def merged(w, low, high):
        whole = w.astype(jnp.float32) + mix_rate * jnp.dot(
            low, high, preferred_element_type=jnp.float32
        )
        return lax.all_gather(whole.astype(jnp.bfloat16), "zero", axis=0, tiled=True).T

    serve_norm = lax.all_gather(
        (norm_train + norm_step).astype(jnp.bfloat16), ("zero", "width"), axis=0, tiled=True
    )
    return merged(w_gate, low_gate, high_gate), merged(w_up, low_up, high_up), serve_norm


def solution(mesh):
    n_zero, n_width = mesh.shape["zero"], mesh.shape["width"]
    planar = n_zero == 2 * 2 * 2 and n_width & (n_width - 1) == 0
    body = functools.partial(by_kernels, n_zero, n_width) if planar else by_gathers
    placed = (
        P("zero", "width"),
        P("zero", None),
        P(None, "width"),
        P("zero", "width"),
        P("zero", None),
        P(None, "width"),
        P(("zero", "width")),
        P(("zero", "width")),
    )
    return jax.shard_map(
        body,
        mesh=mesh,
        in_specs=placed,
        out_specs=(P("width", None), P("width", None), P()),
        check_vma=False,
    )
```

```python
import functools

import jax
import jax.numpy as jnp
from jax import lax
from jax.experimental import pallas as pl
from jax.experimental.pallas import tpu as pltpu
from jax.sharding import PartitionSpec as P

mix_rate = 1.0
MESH = pl.DeviceIdType.MESH
PIECES = 4


def merge_kernel(
    n_zero, n_width, w_gate, low_gate, high_gate, w_up, low_up, high_up, step_a, step_b,
    held, gains, w, low, high, load_sem, gain_send, gain_recv, send_sem, recv_sem,
):
    zero, width = lax.axis_index("zero"), lax.axis_index("width")
    core = lax.rem(zero, 2)
    partner = zero + 1 - 2 * core
    chip = zero // 2
    cx, cy = lax.rem(chip, 2), chip // 2
    over_x = zero + 2 * (1 - 2 * cx)
    over_y = zero + 4 * (1 - 2 * cy)
    first = over_x + core * (over_y - over_x)
    second = over_y + core * (over_x - over_y)
    across = over_x + over_y - zero
    their_first = second + partner - zero
    their_second = first + partner - zero
    their_across = across + partner - zero

    flat = zero * n_width + width
    spans = [1 << b for b in range(n_width.bit_length() - 1)]

    def beside(span):
        return width + span * (1 - 2 * lax.rem(width // span, 2))

    barrier = pltpu.get_barrier_semaphore()
    for target in (partner, first, second):
        pl.semaphore_signal(barrier, inc=1, device_id={"zero": target}, device_id_type=MESH)
    for span in spans:
        pl.semaphore_signal(barrier, inc=1, device_id={"width": beside(span)}, device_id_type=MESH)

    piece = w.shape[2] // PIECES
    parts = [pl.ds(i * piece, piece) for i in range(PIECES)]
    loads = [
        pltpu.make_async_copy(src, dst, load_sem.at[i])
        for i, (src, dst) in enumerate(
            [
                (low_gate, low.at[0]), (high_gate, high.at[0]),
                *[(w_gate.at[:, part], w.at[0, :, part]) for part in parts],
                (low_up, low.at[1]), (high_up, high.at[1]), (w_up, w.at[1]),
            ]
        )
    ]
    for load in loads:
        load.start()
    gains[flat] = step_a[...] + step_b[...]
    for load in loads[:3]:
        load.wait()

    rows = held.shape[2]
    per = PIECES
    chunk = rows // per
    count = 2 * per

    def at(block, i):
        return held.at[block, i // per, pl.ds(pl.multiple_of(lax.rem(i, per) * chunk, chunk), chunk)]

    def make(i):
        a = i // per
        cols = pl.ds(pl.multiple_of(lax.rem(i, per) * chunk, chunk), chunk)
        delta = lax.dot_general(
            high[a, :, cols], low[a], (((0,), (0,)), ((), ())),
            preferred_element_type=jnp.float32,
        )
        base = w[a, :, cols].T.astype(jnp.float32)
        held[zero, a, cols] = (base + mix_rate * delta).astype(held.dtype)

    def copy(flow, block, i, target):
        return pltpu.make_async_remote_copy(
            src_ref=at(block, i), dst_ref=at(block, i),
            send_sem=send_sem.at[flow, i], recv_sem=recv_sem.at[flow, i],
            device_id={"zero": target}, device_id_type=MESH,
        )

    def send_own(i):
        copy(1, zero, i, first).start()
        copy(2, zero, i, second).start()
        copy(0, zero, i, partner).start()

    make(0)
    loads[3].wait()
    make(1)
    pl.semaphore_wait(barrier, 3 + len(spans))
    send_own(0)
    for load in loads[4:]:
        load.wait()

    def make_and_send(i, _):
        make(i)
        send_own(i - 1)
        return _

    lax.fori_loop(2, count, make_and_send, 0)
    send_own(count - 1)

    def gain_beside(b, start):
        span = spans[b]
        own = gains.at[pl.ds(start // span * span, span)]
        return pltpu.make_async_remote_copy(
            src_ref=own, dst_ref=own, send_sem=gain_send.at[b], recv_sem=gain_recv.at[b],
            device_id={"width": beside(span)}, device_id_type=MESH,
        )

    for b, span in enumerate(spans):
        gain_beside(b, flat).start()
        gain_beside(b, zero * n_width + beside(span)).wait_recv()

    def gain_copy(flow, block, target):
        part = gains.at[pl.ds(block * n_width, n_width)]
        return pltpu.make_async_remote_copy(
            src_ref=part, dst_ref=part,
            send_sem=send_sem.at[flow, count], recv_sem=recv_sem.at[flow, count],
            device_id={"zero": target}, device_id_type=MESH,
        )

    gain_copy(1, zero, first).start()
    gain_copy(2, zero, second).start()
    gain_copy(0, zero, partner).start()

    def relay(i, _):
        copy(1, first, i, first).wait_recv()
        copy(3, first, i, second).start()
        copy(4, first, i, partner).start()
        copy(2, second, i, second).wait_recv()
        copy(5, second, i, partner).start()
        return _

    lax.fori_loop(0, count, relay, 0)
    gain_copy(1, first, first).wait_recv()
    gain_copy(3, first, second).start()
    gain_copy(4, first, partner).start()
    gain_copy(2, second, second).wait_recv()
    gain_copy(5, second, partner).start()

    def pass_on(i, _):
        copy(3, across, i, second).wait_recv()
        copy(6, across, i, partner).start()
        return _

    lax.fori_loop(0, count, pass_on, 0)
    gain_copy(3, across, second).wait_recv()
    gain_copy(6, across, partner).start()

    for flow, block in ((0, partner), (4, their_first), (5, their_second), (6, their_across)):
        gain_copy(flow, block, partner).wait_recv()
    for flow, block in enumerate((zero, zero, zero, first, first, second, across)):
        gain_copy(flow, block, partner).wait_send()
    for b in range(len(spans)):
        gain_beside(b, flat).wait_send()

    def end(i, _):
        copy(0, partner, i, partner).wait_recv()
        copy(4, their_first, i, partner).wait_recv()
        copy(5, their_second, i, partner).wait_recv()
        copy(6, their_across, i, partner).wait_recv()
        copy(0, zero, i, partner).wait_send()
        copy(1, zero, i, first).wait_send()
        copy(2, zero, i, second).wait_send()
        copy(3, first, i, second).wait_send()
        copy(4, first, i, partner).wait_send()
        copy(5, second, i, partner).wait_send()
        copy(6, across, i, partner).wait_send()
        return _

    lax.fori_loop(0, count, end, 0)


def flush_kernel(held, out_gate, out_up, sem):
    blocks, _, _, depth = held.shape
    copies = [
        pltpu.make_async_copy(
            held.at[b, a], out.at[:, pl.ds(b * depth, depth)], sem.at[b, a]
        )
        for a, out in enumerate((out_gate, out_up))
        for b in range(blocks)
    ]
    for c in copies:
        c.start()
    for c in copies:
        c.wait()


def by_kernels(n_zero, n_width, w_gate, low_gate, high_gate, w_up, low_up, high_up, norm_train, norm_step):
    depth, rows = w_gate.shape
    rank = high_gate.shape[0]
    share = norm_train.shape[0]
    n = n_zero * n_width
    count = 2 * PIECES
    anywhere = pl.BlockSpec(memory_space=pl.ANY)
    vmem = pl.BlockSpec(memory_space=pltpu.VMEM)
    dma = pltpu.SemaphoreType.DMA
    held, gains = pl.pallas_call(
        functools.partial(merge_kernel, n_zero, n_width),
        out_shape=(
            pltpu.VMEM((n_zero, 2, rows, depth), jnp.bfloat16),
            pltpu.VMEM((n, 1, share), jnp.float32),
        ),
        in_specs=[anywhere] * 6 + [vmem] * 2,
        out_specs=(vmem, vmem),
        scratch_shapes=[
            pltpu.VMEM((2, depth, rows), jnp.bfloat16),
            pltpu.VMEM((2, rank, depth), jnp.bfloat16),
            pltpu.VMEM((2, rank, rows), jnp.bfloat16),
            dma((5 + PIECES,)),
            dma((n_width.bit_length(),)),
            dma((n_width.bit_length(),)),
            dma((7, count + 1)),
            dma((7, count + 1)),
        ],
        compiler_params=pltpu.CompilerParams(
            collective_id=0, has_side_effects=True, vmem_limit_bytes=34 * 2**20
        ),
    )(
        w_gate, low_gate.T, high_gate, w_up, low_up.T, high_up,
        norm_train.reshape(1, share), norm_step.reshape(1, share),
    )
    out = jax.ShapeDtypeStruct((rows, n_zero * depth), jnp.bfloat16)
    serving_gate, serving_up = pl.pallas_call(
        flush_kernel,
        out_shape=(out, out),
        in_specs=[vmem],
        out_specs=(anywhere, anywhere),
        scratch_shapes=[dma((n_zero, 2))],
        compiler_params=pltpu.CompilerParams(vmem_limit_bytes=34 * 2**20),
    )(pltpu.with_memory_space_constraint(held, pltpu.VMEM))
    return serving_gate, serving_up, gains.reshape(n * share).astype(jnp.bfloat16)


def by_gathers(w_gate, low_gate, high_gate, w_up, low_up, high_up, norm_train, norm_step):
    def merged(w, low, high):
        whole = w.astype(jnp.float32) + mix_rate * jnp.dot(
            low, high, preferred_element_type=jnp.float32
        )
        return lax.all_gather(whole.astype(jnp.bfloat16), "zero", axis=0, tiled=True).T

    serve_norm = lax.all_gather(
        (norm_train + norm_step).astype(jnp.bfloat16), ("zero", "width"), axis=0, tiled=True
    )
    return merged(w_gate, low_gate, high_gate), merged(w_up, low_up, high_up), serve_norm


def solution(mesh):
    n_zero, n_width = mesh.shape["zero"], mesh.shape["width"]
    planar = n_zero == 2 * 2 * 2 and n_width & (n_width - 1) == 0
    body = functools.partial(by_kernels, n_zero, n_width) if planar else by_gathers
    placed = (
        P("zero", "width"),
        P("zero", None),
        P(None, "width"),
        P("zero", "width"),
        P("zero", None),
        P(None, "width"),
        P(("zero", "width")),
        P(("zero", "width")),
    )
    return jax.shard_map(
        body,
        mesh=mesh,
        in_specs=placed,
        out_specs=(P("width", None), P("width", None), P()),
        check_vma=False,
    )
```
